32 devices in a mesh: dp: 2 (over x), expert: 4 (over z), mp: 4 (over y, core).
Axes of the slice: x: 2, y: 2, z: 4, core: 2. Of those that a mesh axis runs over, the one named last changes fastest.
Arguments:
- tokens: bfloat16 [512, 4096], P('dp', ('expert', 'mp')), may hold values from -6 to 6
- expert_index: int32 [512, 2], P('dp'), may hold values from 0 to 3, as said below
- slot_index: int32 [512, 2], P('dp'), may hold values from 0 to 191, as said below
- norm_gain: float32 [4096], P(('expert', 'mp')), may hold values from 0.1 to 1.9
- router_weight: bfloat16 [4, 4096], P(None, ('expert', 'mp')), may hold values from -8 to 8
- gate_weight: bfloat16 [4, 7168, 4096], P('expert', ('dp', 'mp')), may hold values from -0.09375 to 0.09375
- up_weight: bfloat16 [4, 7168, 4096], P('expert', ('dp', 'mp')), may hold values from -0.09375 to 0.09375
- down_weight: bfloat16 [4, 7168, 4096], P('expert', ('dp', 'mp')), may hold values from -0.09375 to 0.09375
- final_gain: float32 [4096], replicated, may hold values from 0.1 to 1.9
- head_weight: bfloat16 [16384, 4096], P(('expert', 'mp')), may hold values from -8 to 8
Outputs:
- layer_out: bfloat16 [512, 4096], P('dp', ('expert', 'mp'))
- head_logsum: float32 [512], P('dp')
- router_penalty: float32 [], replicated
- head_penalty: float32 [], replicated
The draws below stay inside these ranges and needn't reach their ends.
Inputs may be any that keep to these rules, and one draw needn't show every extreme that they name: `expert_index`: each row names 2 different experts. In each aligned block of 256 rows every expert is named at least once and at most 192 times; in every block two experts are named exactly 192 times, and one of them is the same expert in all blocks. `slot_index`: within each aligned block of 256 rows, the choices that name one expert hold the slots 0, 1, 2, ... in the order of rows, and within a row in the order of choices.
All inputs are finite; a program needn't handle non-finite values.
Results may differ from the reference program's by a relative error of at most 0.01115.
Values may be sent and summed in bfloat16 or wider, within the bound.
A program may use at most 128 MiB of HBM per device.

```python
import math
import jax
import jax.numpy as jnp
from jax import lax

D = 4096
FF = 7168
VOCAB = 16384
TOP = 2
TOK_DP = 256
EXPERTS = 4
TOKENS = 512
CAPACITY = 192
SLOTS = 384


def routing_tables(key):
    blocks = TOKENS // TOK_DP
    remain = 2 * TOK_DP - 2 * CAPACITY
    others = EXPERTS - 2
    base_count = remain // others
    extra_count = remain % others
    full_expert = jax.random.randint(jax.random.fold_in(key, 5), (), 0, EXPERTS)

    def one_block(block_key):
        key_order = jax.random.fold_in(block_key, 1)
        key_moved = jax.random.fold_in(block_key, 2)
        key_shuffle = jax.random.fold_in(block_key, 3)
        key_swap = jax.random.fold_in(block_key, 4)
        rest_order = 1 + jax.random.permutation(key_order, EXPERTS - 1).astype(jnp.int32)
        rank_expert = (full_expert + jnp.concatenate([jnp.zeros((1,), jnp.int32), rest_order])) % EXPERTS
        rank_ids = jnp.arange(others, dtype=jnp.int32)
        counts_rest = base_count + (rank_ids < extra_count).astype(jnp.int32)
        moved_count = jax.random.randint(key_moved, (others,), 0, base_count // 4 + 1)
        counts_rest = counts_rest - moved_count + jnp.roll(moved_count, 1)
        counts = jnp.concatenate([jnp.full((2,), CAPACITY, jnp.int32), counts_rest])
        bounds = jnp.cumsum(counts)
        places = jnp.arange(2 * TOK_DP, dtype=jnp.int32)
        rank_of = jnp.sum((places[:, None] >= bounds[None, :]).astype(jnp.int32), axis=1)
        labels = rank_expert[rank_of]
        choice_pairs = jnp.stack([labels[:TOK_DP], labels[TOK_DP:]], axis=1)
        shuffle = jax.random.permutation(key_shuffle, TOK_DP)
        choice_pairs = choice_pairs[shuffle]
        swap_order = jax.random.randint(key_swap, (TOK_DP, 1), 0, 2)
        choice_pairs = jnp.where(swap_order == 1, choice_pairs[:, ::-1], choice_pairs)
        flat_pairs = choice_pairs.reshape(-1)
        hit_table = (flat_pairs[:, None] == jnp.arange(EXPERTS, dtype=jnp.int32)[None, :]).astype(jnp.int32)
        running = jnp.cumsum(hit_table, axis=0)
        slot_table = jnp.sum(hit_table * running, axis=1) - 1
        return (choice_pairs.astype(jnp.int32), slot_table.reshape(TOK_DP, 2).astype(jnp.int32))
    block_keys = jax.random.split(jax.random.fold_in(key, 7), blocks)
    chosen, slotted = jax.vmap(one_block)(block_keys)
    return (chosen.reshape(TOKENS, 2), slotted.reshape(TOKENS, 2))


def draw_expert_index(key, part):
    return routing_tables(jax.random.fold_in(key, 11))[0]


def draw_slot_index(key, part):
    return routing_tables(jax.random.fold_in(key, 11))[1]


def drawn_rows(key, rows, width, scale):
    base_key = jax.random.fold_in(key, 1)
    values = jax.random.normal(base_key, (rows, width), jnp.float32) * scale
    return jnp.clip(values, -8.0, 8.0).astype(jnp.bfloat16)


def draw_router_weight(key, part):
    return drawn_rows(jax.random.fold_in(key, 21), EXPERTS, D, 1.0 / math.sqrt(D))


def draw_head_weight(key, part):
    return drawn_rows(jax.random.fold_in(key, 31), VOCAB, D, 3.0 / math.sqrt(D))


def with_spikes(drawn, own_key, source, target, blocks, factor):
    owner, partner = [(jnp.arange(drawn.shape[dim]) // (drawn.shape[dim] // blocks)).reshape([-1 if axis == dim else 1 for axis in range(drawn.ndim)]) for dim in (source, target)]
    chosen = jax.random.permutation(own_key, blocks)[partner]
    strong = (owner == chosen) | (owner == (partner + blocks // 2) % blocks)
    return jnp.where(strong, factor * drawn, drawn)


def steps_of(own_key, extent, pieces, least, top_value):
    level, own = 1.0, jax.random.fold_in(own_key, 6)
    for axis_at, parts in pieces:
        draws = jnp.exp(jax.random.uniform(jax.random.fold_in(own, axis_at), (parts,), jnp.float32, least / len(pieces), top_value / len(pieces)))
        level = level * jnp.repeat(draws, extent[axis_at] // parts).reshape([-1 if axis == axis_at else 1 for axis in range(len(extent))])
    return level


def noise(own_key, dims, deviation, bound, cuts=(), held_as=jnp.bfloat16):
    array = jax.random.normal(own_key, dims, jnp.float32) * deviation
    if len(cuts) > 0:
        array = steps_of(own_key, dims, cuts, -0.22, 0.18) * array
    return jnp.clip(array, min=-bound, max=bound).astype(held_as)


def noise_with(key, shape, scale, limit, shards, heavy, kind=jnp.bfloat16):
    values = scale * jax.random.normal(key, shape, jnp.float32)
    if shards:
        values = values * steps_of(key, shape, shards, -0.22, 0.18)
    return jnp.clip(with_spikes(values, jax.random.fold_in(key, 3), *heavy), -limit, limit).astype(kind)


def setup_inputs(seed: int = 0) -> dict:
    arg_keys = jax.random.split(jax.random.key(seed), 11)
    return {
        "tokens": noise(arg_keys[0], (TOKENS, D), 1.0, 6.0, ((0, 2), (1, 16))),
        "expert_index": draw_expert_index(jax.random.fold_in(arg_keys[10], 71), 0),
        "slot_index": draw_slot_index(jax.random.fold_in(arg_keys[10], 71), 0),
        "norm_gain": jnp.clip(1.0 + 0.18 * jax.random.normal(arg_keys[3], (D,), jnp.float32), 0.1, 1.9),
        "router_weight": draw_router_weight(jax.random.fold_in(arg_keys[10], 71), 0),
        "gate_weight": noise(arg_keys[5], (EXPERTS, FF, D), D ** -0.5, 0.09375, ((0, 4), (1, 8))),
        "up_weight": noise(arg_keys[6], (EXPERTS, FF, D), D ** -0.5, 0.09375, ((0, 4), (1, 8))),
        "down_weight": noise_with(arg_keys[7], (EXPERTS, FF, D), FF ** -0.5, 0.09375, ((0, 4), (1, 8)), (1, 2, 8, 2.0)),
        "final_gain": jnp.clip(1.0 + 0.18 * jax.random.normal(arg_keys[8], (D,), jnp.float32), 0.1, 1.9),
        "head_weight": draw_head_weight(jax.random.fold_in(arg_keys[10], 71), 0),
    }


epsilon = 1e-05

def run_expert(operands):
    slot_rows, gate_matrix, up_matrix, down_matrix = operands
    gate_value = jnp.dot(slot_rows, gate_matrix.T, preferred_element_type=jnp.float32)
    up_value = jnp.dot(slot_rows, up_matrix.T, preferred_element_type=jnp.float32)
    hidden = (jax.nn.silu(gate_value) * up_value).astype(jnp.bfloat16)
    return jnp.dot(hidden, down_matrix, preferred_element_type=jnp.float32).astype(jnp.bfloat16)

def reference(tokens, expert_index, slot_index, norm_gain, router_weight, gate_weight, up_weight, down_weight, final_gain, head_weight):
    tokens_float = tokens.astype(jnp.float32)
    inverse = lax.rsqrt(lax.optimization_barrier(jnp.mean(tokens_float * tokens_float, axis=1)) + epsilon)
    normed = tokens_float * inverse[:, None] * norm_gain[None, :]
    normed_rows = normed.astype(jnp.bfloat16)
    router_logits = jnp.dot(normed, router_weight.astype(jnp.float32).T, precision=lax.Precision.HIGHEST)
    router_logsum = jax.nn.logsumexp(router_logits, axis=1)
    picked = jnp.take_along_axis(router_logits, expert_index, axis=1)
    gate_weights = jax.nn.softmax(picked, axis=1)
    shard_number = jnp.arange(TOKENS, dtype=jnp.int32) // TOK_DP
    position = shard_number[:, None] * CAPACITY + slot_index
    buffer = jnp.zeros((EXPERTS, SLOTS, D), jnp.bfloat16)
    buffer = buffer.at[expert_index.reshape(-1), position.reshape(-1)].set(jnp.repeat(normed_rows, TOP, axis=0))
    outputs = lax.map(run_expert, (buffer, gate_weight, up_weight, down_weight))
    picked_rows = outputs[expert_index, position]
    combined = lax.optimization_barrier(jnp.sum(gate_weights[:, :, None] * picked_rows.astype(jnp.float32), axis=1))
    layer_out = (tokens_float + combined).astype(jnp.bfloat16)
    layer_float = layer_out.astype(jnp.float32)
    head_scale = lax.rsqrt(lax.optimization_barrier(jnp.mean(layer_float * layer_float, axis=1)) + epsilon)
    head_in = (layer_float * head_scale[:, None] * final_gain[None, :]).astype(jnp.bfloat16)
    logits = jnp.dot(head_in, head_weight.T, preferred_element_type=jnp.float32)
    head_logsum = jax.nn.logsumexp(logits, axis=1)
    return (layer_out, head_logsum, jnp.mean(router_logsum * router_logsum), jnp.mean(head_logsum * head_logsum))
```

```python
import functools
import jax
import jax.numpy as jnp
from jax import lax
from jax.experimental import pallas as pl
from jax.experimental.pallas import tpu as pltpu
from jax.sharding import PartitionSpec as P

epsilon = 1e-05
MESH = pl.DeviceIdType.MESH
F32 = jnp.float32
BF16 = jnp.bfloat16
NT = (((1,), (1,)), ((), ()))
VMEM_LIMIT = 64 * 1024 * 1024 - 65536


def remote(src, dst, send_sem, recv_sem, device):
    return pltpu.make_async_remote_copy(
        src_ref=src,
        dst_ref=dst,
        send_sem=send_sem,
        recv_sem=recv_sem,
        device_id=device,
        device_id_type=MESH,
    )


def greet(devices):
    barrier = pltpu.get_barrier_semaphore()
    for device in devices:
        pl.semaphore_signal(barrier, inc=1, device_id=device, device_id_type=MESH)
    pl.semaphore_wait(barrier, len(devices))


def arrival_order(count):
    order = [0]
    for step in range(1, count // 2 + 1):
        order.append(step)
        if count - step != step:
            order.append(count - step)
    return order[:count]


class Place:
    def __init__(self, sizes):
        self.X, self.Z, self.MP = sizes
        self.C = 2 if self.MP % 2 == 0 else 1
        self.Y = self.MP // self.C
        self.x = lax.axis_index("dp")
        self.z = lax.axis_index("expert")
        self.m = lax.axis_index("mp")
        self.y = self.m // self.C
        self.c = lax.rem(self.m, self.C)
        self.linear = self.z * self.MP + self.m
        self.swap = self.X == self.Y
        self.first = (1 - self.c) if self.swap else 1
        self.S1, self.S2 = self.X, self.Y

    def plane_peer(self, j):
        other = lax.rem(self.linear + j, self.Z * self.MP)
        return (self.x, other // self.MP, lax.rem(other, self.MP))

    def z_peer(self, j):
        return (self.x, lax.rem(self.z + j, self.Z), self.m)

    def x_peer(self, j):
        return (lax.rem(self.x + j, self.X), self.z, self.m)

    def y_peer(self, j):
        return (self.x, self.z, lax.rem(self.y + j, self.Y) * self.C + self.c)

    def c_peer(self, j):
        return (self.x, self.z, self.y * self.C + lax.rem(self.c + j, self.C))

    def moved(self, first, d1, d2):
        if not self.swap:
            return lax.rem(self.x + d1, self.X), lax.rem(self.y + d2, self.Y)
        return (
            lax.rem(self.x + first * d1 + (1 - first) * d2, self.X),
            lax.rem(self.y + (1 - first) * d1 + first * d2, self.Y),
        )

    def peer(self, d1, d2):
        x, y = self.moved(self.first, d1, d2)
        return (x, self.z, y * self.C + self.c)


def layer_kernel(
    sizes,
    experts,
    top,
    capacity,
    tokens_ref,
    index_ref,
    gain_ref,
    router_ref,
    gate_ref,
    up_ref,
    down_ref,
    out_ref,
    logsum_ref,
    stat,
    stats,
    turned,
    slots,
    rows,
    wgu,
    wd,
    hidden,
    part,
    got_c,
    sum_c,
    got_p,
    sum_p,
    got_q,
    final,
    back,
    stat_send,
    stat_recv,
    own_sem,
    z_send,
    z_recv,
    g_send,
    g_recv,
    w_sem,
    c_send,
    c_recv,
    p_send,
    p_recv,
    q_send,
    q_recv,
    r_send,
    r_recv,
):
    place = Place(sizes)
    X, Z, MP, Y, C = place.X, place.Z, place.MP, place.Y, place.C
    S1, S2 = place.S1, place.S2
    x, z, m, c = place.x, place.z, place.m, place.c
    N = Z * MP
    count, lf = tokens_ref.shape
    width = N * lf
    tiles, _, tile, _ = wgu.shape
    padded = router_ref.shape[0]

    weight_copies = []
    for t in range(tiles):
        for which, source in ((0, gate_ref), (1, up_ref)):
            weight_copies.append(
                pltpu.make_async_copy(
                    source.at[pl.ds(t * tile, tile), :], wgu.at[t, which], w_sem.at[2 * t + which]
                )
            )
    down_copy = pltpu.make_async_copy(down_ref, wd, w_sem.at[2 * tiles])
    for copy in weight_copies:
        copy.start()
    down_copy.start()

    tok = tokens_ref[...].astype(F32)
    gained = tok * gain_ref[...]
    high = lax.Precision.HIGHEST
    stat[0:padded] = lax.dot_general(
        router_ref[...], gained, NT, precision=high, preferred_element_type=F32
    )
    stat[padded : padded + 8] = lax.dot_general(
        jnp.ones((8, lf), F32), tok * tok, NT, precision=high, preferred_element_type=F32
    )
    stats[pl.ds(place.linear, 1)] = stat[...][None]

    greet(
        [place.plane_peer(j) for j in range(1, N)] + [place.x_peer(j) for j in range(1, X)]
    )

    sends = []
    for j in range(1, N):
        copy = remote(
            stat, stats.at[place.linear], stat_send.at[j], stat_recv.at[j], place.plane_peer(j)
        )
        copy.start()
        sends.append(copy)
    for copy in sends:
        copy.wait_recv()

    total = stats[0]
    for j in range(1, N):
        total = total + stats[j]
    inverse = lax.rsqrt(total[padded : padded + 1] / width + epsilon)
    logits = total[0:experts] * inverse
    peak = jnp.max(logits, axis=0, keepdims=True)
    logsum_ref[...] = peak + jnp.log(jnp.sum(jnp.exp(logits - peak), axis=0, keepdims=True))
    index = index_ref[...]
    numbers = lax.broadcasted_iota(jnp.int32, (experts, count), 0)
    picked = [
        jnp.sum(jnp.where(numbers == index[k : k + 1], logits, 0.0), axis=0, keepdims=True)
        for k in range(top)
    ]
    top_peak = functools.reduce(jnp.maximum, picked)
    raised = [jnp.exp(value - top_peak) for value in picked]
    weight_sum = functools.reduce(jnp.add, raised)
    turned[...] = jnp.zeros_like(turned)
    turned[0:1] = inverse
    for k in range(top):
        turned[1 + k : 2 + k] = raised[k] / weight_sum
        turned[1 + top + k : 2 + top + k] = index[top + k : top + k + 1].astype(F32)
    columns = jnp.transpose(turned[...])

    normed = (gained * columns[:, 0:1]).astype(BF16)
    for e in range(experts):
        every = lax.broadcasted_iota(jnp.int32, (capacity, count), 0) + e * capacity
        chosen = every == index[top : top + 1]
        for k in range(1, top):
            chosen = jnp.logical_or(chosen, every == index[top + k : top + k + 1])
        slots[e] = jnp.dot(
            jnp.where(chosen, 1.0, 0.0).astype(BF16), normed, preferred_element_type=F32
        ).astype(BF16)

    def block(sx, sz, sm):
        return rows.at[
            pl.ds(pl.multiple_of(sx * capacity, capacity), capacity),
            pl.ds(pl.multiple_of((sz * MP + sm) * lf, lf), lf),
        ]

    order = arrival_order(Z)
    own = pltpu.make_async_copy(slots.at[z], block(x, z, m), own_sem.at[0])
    own.start()
    z_copies = {}
    for j in order[1:]:
        copy = remote(
            slots.at[lax.rem(z + j, Z)], block(x, z, m), z_send.at[j], z_recv.at[j], place.z_peer(j)
        )
        copy.start()
        sends.append(copy)
        z_copies[j] = copy

    def sem_at(k, d1, d2, dc):
        return ((k * S1 + d1) * S2 + d2) * C + dc

    def source(k, d1, d2, dc):
        sc = lax.rem(c + C - dc, C)
        first = (1 - sc) if place.swap else 1
        sx, sy = place.moved(first, lax.rem(S1 - d1, S1), lax.rem(S2 - d2, S2))
        return block(sx, lax.rem(z + Z - k, Z), sy * C + sc)

    def forward(k, d1, d2, axis):
        held = source(k, d1, d2, 0)
        if axis == 0:
            targets = [((d, d2, 0), place.peer(d, 0)) for d in range(1, S1)]
        elif axis == 1:
            targets = [((d1, d, 0), place.peer(0, d)) for d in range(1, S2)]
        else:
            targets = [((d1, d2, d), place.c_peer(d)) for d in range(1, C)]
        for spot, device in targets:
            at = sem_at(k, *spot)
            copy = remote(held, held, g_send.at[at], g_recv.at[at], device)
            copy.start()
            sends.append(copy)

    def wait_for(k, d1, d2, dc):
        held = source(k, d1, d2, dc)
        at = sem_at(k, d1, d2, dc)
        remote(held, held, g_send.at[at], g_recv.at[at], place.z_peer(1)).wait_recv()

    def hop_own(k):
        if k == 0:
            own.wait()
        else:
            z_copies[k].wait_recv()
        forward(k, 0, 0, 0)
        forward(k, 0, 0, 1)
        forward(k, 0, 0, 2)

    def hop_first(k):
        for d in range(1, S1):
            wait_for(k, d, 0, 0)
            forward(k, d, 0, 1)
            forward(k, d, 0, 2)
        for d in range(1, S2):
            wait_for(k, 0, d, 0)
            forward(k, 0, d, 2)

    def hop_second(k):
        for d1 in range(1, S1):
            for d2 in range(1, S2):
                wait_for(k, d1, d2, 0)
                forward(k, d1, d2, 2)

    for step in range(Z + 2):
        if step < Z:
            hop_own(order[step])
        if 0 <= step - 1 < Z:
            hop_first(order[step - 1])
        if 0 <= step - 2 < Z:
            hop_second(order[step - 2])
    for k in order:
        for d1 in range(S1):
            for d2 in range(S2):
                for dc in range(1, C):
                    wait_for(k, d1, d2, dc)

    for copy in weight_copies:
        copy.wait()

    if tile % 128 == 0:

        def expert_tile(t, carry):
            both = lax.dot_general(
                rows[...], wgu[t].reshape(2 * tile, width), NT, preferred_element_type=F32
            )
            gate_value, up_value = both[:, :tile], both[:, tile:]
            value = gate_value / (1.0 + jnp.exp(-gate_value)) * up_value
            hidden[:, pl.ds(pl.multiple_of(t * tile, tile), tile)] = value.astype(BF16)
            return carry

        lax.fori_loop(0, tiles, expert_tile, 0)
    else:
        for t in range(tiles):
            gate_value = lax.dot_general(rows[...], wgu[t, 0], NT, preferred_element_type=F32)
            up_value = lax.dot_general(rows[...], wgu[t, 1], NT, preferred_element_type=F32)
            value = gate_value / (1.0 + jnp.exp(-gate_value)) * up_value
            hidden[:, t * tile : (t + 1) * tile] = value.astype(BF16)

    down_copy.wait()
    back_order = order[1:] + [0]
    c_copies, p_copies, q_copies, r_copies = {}, {}, {}, {}

    def down_block(k, ty, dc):
        tz = lax.rem(z + k, Z)
        tm = ty * C + lax.rem(c + dc, C)
        at = pl.multiple_of((tz * MP + tm) * lf, lf)
        part[k, ty, dc] = jnp.dot(
            hidden[...], wd[:, pl.ds(at, lf)], preferred_element_type=F32
        ).astype(BF16)

    def stage_down(k):
        for dc in list(range(1, C)) + [0]:

            def one(ty, carry, dc=dc):
                down_block(k, ty, dc)
                return carry

            lax.fori_loop(0, Y, one, 0)
            if dc:
                copy = remote(
                    part.at[k, :, dc],
                    got_c.at[k, dc],
                    c_send.at[k * C + dc],
                    c_recv.at[k * C + dc],
                    place.c_peer(dc),
                )
                copy.start()
                sends.append(copy)
                c_copies[k, dc] = copy

    def stage_c(k):
        value = part[k, :, 0].astype(F32)
        for dc in range(1, C):
            c_copies[k, dc].wait_recv()
            value = value + got_c[k, dc].astype(F32)
        sum_c[k] = value.astype(BF16)
        for i in range(1, S2):
            for d1 in range(S1):
                tx, ty = place.moved(place.first, d1, i)
                at = (k * S2 + i) * S1 + d1
                copy = remote(
                    sum_c.at[k, ty, pl.ds(pl.multiple_of(tx * capacity, capacity), capacity)],
                    got_p.at[k, i, d1],
                    p_send.at[at],
                    p_recv.at[at],
                    place.peer(0, i),
                )
                copy.start()
                sends.append(copy)
                p_copies[k, i, d1] = copy

    def stage_p(k):
        for d1 in list(range(1, S1)) + [0]:
            tx, ty = place.moved(place.first, d1, 0)
            value = sum_c[
                k, ty, pl.ds(pl.multiple_of(tx * capacity, capacity), capacity)
            ].astype(F32)
            for i in range(1, S2):
                p_copies[k, i, d1].wait_recv()
                value = value + got_p[k, i, d1].astype(F32)
            sum_p[k, d1] = value.astype(BF16)
            if d1:
                at = k * S1 + d1
                copy = remote(
                    sum_p.at[k, d1], got_q.at[k, d1], q_send.at[at], q_recv.at[at], place.peer(d1, 0)
                )
                copy.start()
                sends.append(copy)
                q_copies[k, d1] = copy

    def stage_q(k):
        value = sum_p[k, 0].astype(F32)
        for d1 in range(1, S1):
            q_copies[k, d1].wait_recv()
            value = value + got_q[k, d1].astype(F32)
        if k == 0:
            back[pl.ds(z, 1)] = value.astype(BF16)[None]
        else:
            final[k] = value.astype(BF16)
            copy = remote(final.at[k], back.at[z], r_send.at[k], r_recv.at[k], place.z_peer(k))
            copy.start()
            sends.append(copy)
            r_copies[k] = copy

    for step in range(Z + 3):
        if step < Z:
            stage_down(back_order[step])
        if 0 <= step - 1 < Z:
            stage_c(back_order[step - 1])
        if 0 <= step - 2 < Z:
            stage_p(back_order[step - 2])
        if 0 <= step - 3 < Z:
            stage_q(back_order[step - 3])
    for k in order[1:]:
        r_copies[k].wait_recv()

    returned = back[...].reshape(experts * capacity, lf)
    every = lax.broadcasted_iota(jnp.int32, (count, experts * capacity), 1).astype(F32)
    combined = jnp.zeros((count, lf), F32)
    for k in range(top):
        chosen = jnp.where(every == columns[:, 1 + top + k : 2 + top + k], 1.0, 0.0).astype(BF16)
        combined = combined + columns[:, 1 + k : 2 + k] * jnp.dot(
            chosen, returned, preferred_element_type=F32
        )
    out_ref[...] = (tokens_ref[...].astype(F32) + combined).astype(BF16)
    for copy in sends:
        copy.wait_send()


def head_kernel(
    sizes,
    layer_ref,
    router_logsum_ref,
    gain_ref,
    weight_ref,
    logsum_ref,
    penalty_ref,
    full,
    weight,
    head_in,
    logits,
    pair,
    pairs,
    square,
    squares,
    w_sem,
    z_send,
    z_recv,
    g_send,
    g_recv,
    pair_send,
    pair_recv,
    square_send,
    square_recv,
):
    place = Place(sizes)
    X, Z, MP, Y, C = place.X, place.Z, place.MP, place.Y, place.C
    x, z, m, y, c = place.x, place.z, place.m, place.y, place.c
    N = Z * MP
    count, lf = layer_ref.shape
    width = N * lf
    vocabulary = weight_ref.shape[0]

    weight_copy = pltpu.make_async_copy(weight_ref, weight, w_sem.at[0])
    weight_copy.start()
    greet(
        [place.plane_peer(j) for j in range(1, N)] + [place.x_peer(j) for j in range(1, X)]
    )

    def block(sz, sm):
        return full.at[:, pl.ds(pl.multiple_of((sz * MP + sm) * lf, lf), lf)]

    order = arrival_order(Z)
    sends = []
    z_copies = {}
    own = pltpu.make_async_copy(layer_ref, block(z, m), w_sem.at[1])
    own.start()
    for j in order[1:]:
        copy = remote(layer_ref, block(z, m), z_send.at[j], z_recv.at[j], place.z_peer(j))
        copy.start()
        sends.append(copy)
        z_copies[j] = copy

    def sem_at(k, dy, dc):
        return (k * Y + dy) * C + dc

    def source(k, dy, dc):
        sy = lax.rem(y + Y - dy, Y)
        return block(lax.rem(z + Z - k, Z), sy * C + lax.rem(c + C - dc, C))

    def send(k, dy, dc, held, device):
        at = sem_at(k, dy, dc)
        copy = remote(held, held, g_send.at[at], g_recv.at[at], device)
        copy.start()
        sends.append(copy)

    def wait_for(k, dy, dc):
        held = source(k, dy, dc)
        at = sem_at(k, dy, dc)
        remote(held, held, g_send.at[at], g_recv.at[at], place.z_peer(1)).wait_recv()

    def hop_own(k):
        if k == 0:
            own.wait()
        else:
            z_copies[k].wait_recv()
        held = source(k, 0, 0)
        for d in range(1, Y):
            send(k, d, 0, held, place.y_peer(d))
        for d in range(1, C):
            send(k, 0, d, held, place.c_peer(d))

    def hop_y(k):
        for dy in range(1, Y):
            wait_for(k, dy, 0)
            for d in range(1, C):
                send(k, dy, d, source(k, dy, 0), place.c_peer(d))

    for step in range(Z + 1):
        if step < Z:
            hop_own(order[step])
        if step >= 1:
            hop_y(order[step - 1])
    for k in order:
        for dy in range(Y):
            for dc in range(1, C):
                wait_for(k, dy, dc)

    chunk = 32 if count % 32 == 0 else count

    def norm_rows(r, carry):
        at = pl.ds(pl.multiple_of(r * chunk, chunk), chunk)
        value = full[at, :].astype(F32)
        scale = lax.rsqrt(jnp.mean(value * value, axis=1, keepdims=True) + epsilon)
        head_in[at, :] = (value * scale * gain_ref[...]).astype(BF16)
        return carry

    lax.fori_loop(0, count // chunk, norm_rows, 0)
    weight_copy.wait()
    tile = 256 if vocabulary % 256 == 0 else vocabulary

    def vocab_tile(t, peak):
        at = pl.ds(pl.multiple_of(t * tile, tile), tile)
        value = lax.dot_general(weight[at, :], head_in[...], NT, preferred_element_type=F32)
        logits[at, :] = value
        return jnp.maximum(peak, jnp.max(value, axis=0, keepdims=True))

    start = jnp.full((1, count), -jnp.inf, F32)
    peak = lax.fori_loop(0, vocabulary // tile, vocab_tile, start)
    pair[0:1] = peak
    pair[1:2] = jnp.sum(jnp.exp(logits[...] - peak), axis=0, keepdims=True)
    pair[2:8] = jnp.zeros((6, count), F32)
    pairs[pl.ds(place.linear, 1)] = pair[...][None]
    pair_copies = []
    for j in range(1, N):
        copy = remote(
            pair, pairs.at[place.linear], pair_send.at[j], pair_recv.at[j], place.plane_peer(j)
        )
        copy.start()
        pair_copies.append(copy)
    for copy in pair_copies:
        copy.wait_recv()
    everything = pairs[...]
    peaks, totals = everything[:, 0, :], everything[:, 1, :]
    merged = jnp.max(peaks, axis=0, keepdims=True)
    logsum = merged + jnp.log(jnp.sum(totals * jnp.exp(peaks - merged), axis=0, keepdims=True))
    logsum_ref[...] = logsum
    router_logsum = router_logsum_ref[...]
    square[...] = jnp.zeros_like(square)
    square[0:1] = jnp.broadcast_to(
        jnp.sum(router_logsum * router_logsum, axis=1, keepdims=True), (1, square.shape[1])
    )
    square[1:2] = jnp.broadcast_to(
        jnp.sum(logsum * logsum, axis=1, keepdims=True), (1, square.shape[1])
    )
    squares[pl.ds(x, 1)] = square[...][None]
    square_copies = []
    for j in range(1, X):
        copy = remote(
            square, squares.at[x], square_send.at[j], square_recv.at[j], place.x_peer(j)
        )
        copy.start()
        square_copies.append(copy)
    for copy in square_copies:
        copy.wait_recv()
    total = squares[0]
    for j in range(1, X):
        total = total + squares[j]
    penalty_ref[...] = total / (count * X)
    for copy in sends + pair_copies + square_copies:
        copy.wait_send()


def body(
    sizes,
    tokens,
    expert_index,
    slot_index,
    norm_gain,
    router_weight,
    gate_weight,
    up_weight,
    down_weight,
    final_gain,
    head_weight,
):
    X, Z, MP = sizes
    C = 2 if MP % 2 == 0 else 1
    Y = MP // C
    N = Z * MP
    count, lf = tokens.shape
    top = expert_index.shape[1]
    experts = router_weight.shape[0]
    capacity = 3 * count // experts
    _, ff, width = gate_weight.shape
    vocabulary = head_weight.shape[0]
    padded = -(-experts // 8) * 8
    flat = expert_index * capacity + slot_index
    index = jnp.concatenate([expert_index, flat], axis=1).T
    router = jnp.pad(router_weight.astype(F32), ((0, padded - experts), (0, 0)))
    tile = 128 if ff % 128 == 0 else ff
    vmem = pl.BlockSpec(memory_space=pltpu.VMEM)
    anywhere = pl.BlockSpec(memory_space=pl.ANY)
    dma = pltpu.SemaphoreType.DMA
    params = functools.partial(
        pltpu.CompilerParams, has_side_effects=True, vmem_limit_bytes=VMEM_LIMIT
    )
    layer_out, router_logsum = pl.pallas_call(
        functools.partial(layer_kernel, sizes, experts, top, capacity),
        out_shape=(
            jax.ShapeDtypeStruct((count, lf), BF16),
            jax.ShapeDtypeStruct((1, count), F32),
        ),
        in_specs=[vmem] * 4 + [anywhere] * 3,
        out_specs=(vmem, vmem),
        scratch_shapes=[
            pltpu.VMEM((padded + 8, count), F32),
            pltpu.VMEM((N, padded + 8, count), F32),
            pltpu.VMEM((128, count), F32),
            pltpu.VMEM((experts, capacity, lf), BF16),
            pltpu.VMEM((X * capacity, width), BF16),
            pltpu.VMEM((ff // tile, 2, tile, width), BF16),
            pltpu.VMEM((ff, width), BF16),
            pltpu.VMEM((X * capacity, ff), BF16),
            pltpu.VMEM((Z, Y, C, X * capacity, lf), BF16),
            pltpu.VMEM((Z, C, Y, X * capacity, lf), BF16),
            pltpu.VMEM((Z, Y, X * capacity, lf), BF16),
            pltpu.VMEM((Z, Y, X, capacity, lf), BF16),
            pltpu.VMEM((Z, X, capacity, lf), BF16),
            pltpu.VMEM((Z, X, capacity, lf), BF16),
            pltpu.VMEM((Z, capacity, lf), BF16),
            pltpu.VMEM((Z, capacity, lf), BF16),
            dma((N,)),
            dma((N,)),
            dma((1,)),
            dma((Z,)),
            dma((Z,)),
            dma((Z * X * Y * C,)),
            dma((Z * X * Y * C,)),
            dma((2 * (ff // tile) + 1,)),
            dma((Z * C,)),
            dma((Z * C,)),
            dma((Z * X * Y,)),
            dma((Z * X * Y,)),
            dma((Z * X,)),
            dma((Z * X,)),
            dma((Z,)),
            dma((Z,)),
        ],
        compiler_params=params(collective_id=0),
        name="layer",
    )(
        tokens,
        index,
        norm_gain[None, :],
        router,
        gate_weight[0],
        up_weight[0],
        down_weight[0],
    )
    logsum, penalty = pl.pallas_call(
        functools.partial(head_kernel, sizes),
        out_shape=(
            jax.ShapeDtypeStruct((1, count), F32),
            jax.ShapeDtypeStruct((8, 128), F32),
        ),
        in_specs=[vmem] * 3 + [anywhere],
        out_specs=(vmem, vmem),
        scratch_shapes=[
            pltpu.VMEM((count, width), BF16),
            pltpu.VMEM((vocabulary, width), BF16),
            pltpu.VMEM((count, width), BF16),
            pltpu.VMEM((vocabulary, count), F32),
            pltpu.VMEM((8, count), F32),
            pltpu.VMEM((N, 8, count), F32),
            pltpu.VMEM((8, 128), F32),
            pltpu.VMEM((X, 8, 128), F32),
            dma((2,)),
            dma((Z,)),
            dma((Z,)),
            dma((N,)),
            dma((N,)),
            dma((N,)),
            dma((N,)),
            dma((X,)),
            dma((X,)),
        ],
        compiler_params=params(collective_id=1),
        name="head",
    )(layer_out, router_logsum, final_gain[None, :], head_weight)
    return (layer_out, logsum[0], penalty[0, 0], penalty[1, 0])


def solution(mesh):
    in_specs = (
        P("dp", ("expert", "mp")),
        P("dp", None),
        P("dp", None),
        P(("expert", "mp")),
        P(None, ("expert", "mp")),
        P("expert", ("dp", "mp"), None),
        P("expert", ("dp", "mp"), None),
        P("expert", ("dp", "mp"), None),
        P(),
        P(("expert", "mp"), None),
    )
    out_specs = (P("dp", ("expert", "mp")), P("dp"), P(), P())
    sizes = (mesh.shape["dp"], mesh.shape["expert"], mesh.shape["mp"])
    return jax.shard_map(
        functools.partial(body, sizes),
        mesh=mesh,
        in_specs=in_specs,
        out_specs=out_specs,
        check_vma=False,
    )
```

```python
import functools
import jax
import jax.numpy as jnp
from jax import lax
from jax.experimental import pallas as pl
from jax.experimental.pallas import tpu as pltpu
from jax.sharding import PartitionSpec as P

epsilon = 1e-05
MESH = pl.DeviceIdType.MESH
F32 = jnp.float32
BF16 = jnp.bfloat16
NT = (((1,), (1,)), ((), ()))
VMEM_LIMIT = 64 * 1024 * 1024 - 65536


def remote(src, dst, send_sem, recv_sem, device):
    return pltpu.make_async_remote_copy(
        src_ref=src,
        dst_ref=dst,
        send_sem=send_sem,
        recv_sem=recv_sem,
        device_id=device,
        device_id_type=MESH,
    )


def greet(devices):
    barrier = pltpu.get_barrier_semaphore()
    for device in devices:
        pl.semaphore_signal(barrier, inc=1, device_id=device, device_id_type=MESH)
    pl.semaphore_wait(barrier, len(devices))


def arrival_order(count):
    order = [0]
    for step in range(1, count // 2 + 1):
        order.append(step)
        if count - step != step:
            order.append(count - step)
    return order[:count]


class Place:
    def __init__(self, sizes):
        self.X, self.Z, self.MP = sizes
        self.C = 2 if self.MP % 2 == 0 else 1
        self.Y = self.MP // self.C
        self.x = lax.axis_index("dp")
        self.z = lax.axis_index("expert")
        self.m = lax.axis_index("mp")
        self.y = self.m // self.C
        self.c = lax.rem(self.m, self.C)
        self.linear = self.z * self.MP + self.m
        self.swap = self.X == self.Y
        self.first = (1 - self.c) if self.swap else 1
        self.S1, self.S2 = self.X, self.Y

    def plane_peer(self, j):
        other = lax.rem(self.linear + j, self.Z * self.MP)
        return (self.x, other // self.MP, lax.rem(other, self.MP))

    def z_peer(self, j):
        return (self.x, lax.rem(self.z + j, self.Z), self.m)

    def x_peer(self, j):
        return (lax.rem(self.x + j, self.X), self.z, self.m)

    def y_peer(self, j):
        return (self.x, self.z, lax.rem(self.y + j, self.Y) * self.C + self.c)

    def c_peer(self, j):
        return (self.x, self.z, self.y * self.C + lax.rem(self.c + j, self.C))

    def moved(self, first, d1, d2):
        if not self.swap:
            return lax.rem(self.x + d1, self.X), lax.rem(self.y + d2, self.Y)
        return (
            lax.rem(self.x + first * d1 + (1 - first) * d2, self.X),
            lax.rem(self.y + (1 - first) * d1 + first * d2, self.Y),
        )

    def peer(self, d1, d2):
        x, y = self.moved(self.first, d1, d2)
        return (x, self.z, y * self.C + self.c)


def layer_part(
    sizes,
    sends,
    head_weight_copy,
    experts,
    top,
    capacity,
    tokens_ref,
    expert_ref,
    slot_ref,
    gain_ref,
    router_ref,
    gate_ref,
    up_ref,
    down_ref,
    out_ref,
    router,
    flipped,
    acc,
    stat,
    stats,
    turned,
    slots,
    rows,
    wgu,
    wd,
    hidden,
    part,
    got_c,
    sum_c,
    got_p,
    sum_p,
    got_q,
    final,
    back,
    stat_send,
    stat_recv,
    own_sem,
    z_send,
    z_recv,
    g_send,
    g_recv,
    w_sem,
    c_send,
    c_recv,
    p_send,
    p_recv,
    q_send,
    q_recv,
    r_send,
    r_recv,
):
    place = Place(sizes)
    X, Z, MP, Y, C = place.X, place.Z, place.MP, place.Y, place.C
    S1, S2 = place.S1, place.S2
    x, z, m, c = place.x, place.z, place.m, place.c
    N = Z * MP
    count, lf = tokens_ref.shape
    width = N * lf
    tiles, _, tile, _ = wgu.shape

    weight_copies = []
    for t in range(tiles):
        for which, source in ((0, gate_ref), (1, up_ref)):
            weight_copies.append(
                pltpu.make_async_copy(
                    source.at[pl.ds(t * tile, tile), :], wgu.at[t, which], w_sem.at[2 * t + which]
                )
            )
    down_copy = pltpu.make_async_copy(down_ref, wd, w_sem.at[2 * tiles])
    for copy in weight_copies:
        copy.start()
    down_copy.start()
    head_weight_copy.start()

    tok = tokens_ref[...].astype(F32)
    gained = tok * gain_ref[...]
    high = lax.Precision.HIGHEST
    router[...] = jnp.zeros_like(router)
    router[0:experts] = router_ref[...].astype(F32)
    router_part = lax.dot_general(
        router[...], gained, NT, precision=high, preferred_element_type=F32
    )
    square_part = lax.dot_general(
        jnp.ones((8, lf), F32), tok * tok, NT, precision=high, preferred_element_type=F32
    )[0:1]
    line = lax.broadcasted_iota(jnp.int32, stat.shape, 0)
    stat[...] = jnp.where(line == experts, square_part, router_part)
    stats[pl.ds(place.linear, 1)] = stat[...][None]

    greet(
        [place.plane_peer(j) for j in range(1, N)] + [place.x_peer(j) for j in range(1, X)]
    )

    for j in range(1, N):
        copy = remote(
            stat, stats.at[place.linear], stat_send.at[j], stat_recv.at[j], place.plane_peer(j)
        )
        copy.start()
        sends.append(copy)
    flipped[...] = jnp.zeros_like(flipped)
    flipped[:, 0:top] = expert_ref[...].astype(F32)
    flipped[:, top : 2 * top] = (expert_ref[...] * capacity + slot_ref[...]).astype(F32)
    index = jnp.transpose(flipped[...])[0 : 2 * top].astype(jnp.int32)
    for copy in sends:
        copy.wait_recv()

    total = stats[0]
    for j in range(1, N):
        total = total + stats[j]
    inverse = lax.rsqrt(total[experts : experts + 1] / width + epsilon)
    logits = total[0:experts] * inverse
    peak = jnp.max(logits, axis=0, keepdims=True)
    router_logsum = peak + jnp.log(jnp.sum(jnp.exp(logits - peak), axis=0, keepdims=True))
    numbers = lax.broadcasted_iota(jnp.int32, (experts, count), 0)
    picked = [
        jnp.sum(jnp.where(numbers == index[k : k + 1], logits, 0.0), axis=0, keepdims=True)
        for k in range(top)
    ]
    top_peak = functools.reduce(jnp.maximum, picked)
    raised = [jnp.exp(value - top_peak) for value in picked]
    weight_sum = functools.reduce(jnp.add, raised)
    turned[...] = jnp.zeros_like(turned)
    turned[0:1] = inverse
    for k in range(top):
        turned[1 + k : 2 + k] = raised[k] / weight_sum
        turned[1 + top + k : 2 + top + k] = index[top + k : top + k + 1].astype(F32)
    columns = jnp.transpose(turned[...])

    normed = (gained * columns[:, 0:1]).astype(BF16)
    for e in range(experts):
        every = lax.broadcasted_iota(jnp.int32, (capacity, count), 0) + e * capacity
        chosen = every == index[top : top + 1]
        for k in range(1, top):
            chosen = jnp.logical_or(chosen, every == index[top + k : top + k + 1])
        slots[e] = jnp.dot(
            jnp.where(chosen, 1.0, 0.0).astype(BF16), normed, preferred_element_type=F32
        ).astype(BF16)

    def block(sx, sz, sm):
        return rows.at[
            pl.ds(pl.multiple_of(sx * capacity, capacity), capacity),
            pl.ds(pl.multiple_of((sz * MP + sm) * lf, lf), lf),
        ]

    order = arrival_order(Z)
    own = pltpu.make_async_copy(slots.at[z], block(x, z, m), own_sem.at[0])
    own.start()
    z_copies = {}
    for j in order[1:]:
        copy = remote(
            slots.at[lax.rem(z + j, Z)], block(x, z, m), z_send.at[j], z_recv.at[j], place.z_peer(j)
        )
        copy.start()
        sends.append(copy)
        z_copies[j] = copy

    def sem_at(k, d1, d2, dc):
        return ((k * S1 + d1) * S2 + d2) * C + dc

    def source(k, d1, d2, dc):
        sc = lax.rem(c + C - dc, C)
        first = (1 - sc) if place.swap else 1
        sx, sy = place.moved(first, lax.rem(S1 - d1, S1), lax.rem(S2 - d2, S2))
        return block(sx, lax.rem(z + Z - k, Z), sy * C + sc)

    def forward(k, d1, d2, axis):
        held = source(k, d1, d2, 0)
        if axis == 0:
            targets = [((d, d2, 0), place.peer(d, 0)) for d in range(1, S1)]
        elif axis == 1:
            targets = [((d1, d, 0), place.peer(0, d)) for d in range(1, S2)]
        else:
            targets = [((d1, d2, d), place.c_peer(d)) for d in range(1, C)]
        for spot, device in targets:
            at = sem_at(k, *spot)
            copy = remote(held, held, g_send.at[at], g_recv.at[at], device)
            copy.start()
            sends.append(copy)

    def wait_for(k, d1, d2, dc):
        held = source(k, d1, d2, dc)
        at = sem_at(k, d1, d2, dc)
        remote(held, held, g_send.at[at], g_recv.at[at], place.z_peer(1)).wait_recv()

    def hop_own(k):
        if k == 0:
            own.wait()
        else:
            z_copies[k].wait_recv()
        forward(k, 0, 0, 0)
        forward(k, 0, 0, 1)
        forward(k, 0, 0, 2)

    def hop_first(k):
        for d in range(1, S1):
            wait_for(k, d, 0, 0)
            forward(k, d, 0, 1)
            forward(k, d, 0, 2)
        for d in range(1, S2):
            wait_for(k, 0, d, 0)
            forward(k, 0, d, 2)

    def hop_second(k):
        for d1 in range(1, S1):
            for d2 in range(1, S2):
                wait_for(k, d1, d2, 0)
                forward(k, d1, d2, 2)

    def arrive(k):
        for d1 in range(S1):
            for d2 in range(S2):
                for dc in range(1, C):
                    wait_for(k, d1, d2, dc)

    chunk = MP * lf

    def multiply(k, begin, end):
        at = pl.ds(pl.multiple_of(lax.rem(z + Z - k, Z) * chunk, chunk), chunk)

        def expert_tile(t, carry):
            held = rows[:, at]
            if tile % 128 == 0:
                both = lax.dot_general(
                    held,
                    wgu[t, :, :, at].reshape(2 * tile, chunk),
                    NT,
                    preferred_element_type=F32,
                )
                gate_value, up_value = both[:, :tile], both[:, tile:]
            else:
                gate_value = lax.dot_general(held, wgu[t, 0, :, at], NT, preferred_element_type=F32)
                up_value = lax.dot_general(held, wgu[t, 1, :, at], NT, preferred_element_type=F32)
            if not begin:
                gate_value = gate_value + acc[t, 0]
                up_value = up_value + acc[t, 1]
            if end:
                value = gate_value / (1.0 + jnp.exp(-gate_value)) * up_value
                if tiles == 1:
                    hidden[...] = value.astype(BF16)
                else:
                    hidden[:, pl.ds(pl.multiple_of(t * tile, tile), tile)] = value.astype(BF16)
            else:
                acc[t, 0] = gate_value
                acc[t, 1] = up_value
            return carry

        if tiles == 1:
            expert_tile(0, 0)
        else:
            lax.fori_loop(0, tiles, expert_tile, 0)

    for step in range(Z + 3):
        if step < Z:
            hop_own(order[step])
        if 0 <= step - 1 < Z:
            hop_first(order[step - 1])
        if 0 <= step - 2 < Z:
            hop_second(order[step - 2])
        if 0 <= step - 3 < Z:
            if step == 3:
                for copy in weight_copies:
                    copy.wait()
            arrive(order[step - 3])
            multiply(order[step - 3], step == 3, step == Z + 2)

    down_copy.wait()
    back_order = order[1:] + [0]
    c_copies, p_copies, q_copies, r_copies = {}, {}, {}, {}

    def down_block(k, ty, dc):
        tz = lax.rem(z + k, Z)
        tm = ty * C + lax.rem(c + dc, C)
        at = pl.multiple_of((tz * MP + tm) * lf, lf)
        part[k, ty, dc] = jnp.dot(
            hidden[...], wd[:, pl.ds(at, lf)], preferred_element_type=F32
        ).astype(BF16)

    def stage_down(k):
        for dc in list(range(1, C)) + [0]:

            def one(ty, carry, dc=dc):
                down_block(k, ty, dc)
                return carry

            lax.fori_loop(0, Y, one, 0)
            if dc:
                copy = remote(
                    part.at[k, :, dc],
                    got_c.at[k, dc],
                    c_send.at[k * C + dc],
                    c_recv.at[k * C + dc],
                    place.c_peer(dc),
                )
                copy.start()
                sends.append(copy)
                c_copies[k, dc] = copy

    def stage_c(k):
        value = part[k, :, 0].astype(F32)
        for dc in range(1, C):
            c_copies[k, dc].wait_recv()
            value = value + got_c[k, dc].astype(F32)
        sum_c[k] = value.astype(BF16)
        for i in range(1, S2):
            for d1 in range(S1):
                tx, ty = place.moved(place.first, d1, i)
                at = (k * S2 + i) * S1 + d1
                copy = remote(
                    sum_c.at[k, ty, pl.ds(pl.multiple_of(tx * capacity, capacity), capacity)],
                    got_p.at[k, i, d1],
                    p_send.at[at],
                    p_recv.at[at],
                    place.peer(0, i),
                )
                copy.start()
                sends.append(copy)
                p_copies[k, i, d1] = copy

    def stage_p(k):
        for d1 in list(range(1, S1)) + [0]:
            tx, ty = place.moved(place.first, d1, 0)
            value = sum_c[
                k, ty, pl.ds(pl.multiple_of(tx * capacity, capacity), capacity)
            ].astype(F32)
            for i in range(1, S2):
                p_copies[k, i, d1].wait_recv()
                value = value + got_p[k, i, d1].astype(F32)
            sum_p[k, d1] = value.astype(BF16)
            if d1:
                at = k * S1 + d1
                copy = remote(
                    sum_p.at[k, d1], got_q.at[k, d1], q_send.at[at], q_recv.at[at], place.peer(d1, 0)
                )
                copy.start()
                sends.append(copy)
                q_copies[k, d1] = copy

    def stage_q(k):
        value = sum_p[k, 0].astype(F32)
        for d1 in range(1, S1):
            q_copies[k, d1].wait_recv()
            value = value + got_q[k, d1].astype(F32)
        if k == 0:
            back[pl.ds(z, 1)] = value.astype(BF16)[None]
        else:
            final[k] = value.astype(BF16)
            copy = remote(final.at[k], back.at[z], r_send.at[k], r_recv.at[k], place.z_peer(k))
            copy.start()
            sends.append(copy)
            r_copies[k] = copy

    for step in range(Z + 3):
        if step < Z:
            stage_down(back_order[step])
        if 0 <= step - 1 < Z:
            stage_c(back_order[step - 1])
        if 0 <= step - 2 < Z:
            stage_p(back_order[step - 2])
        if 0 <= step - 3 < Z:
            stage_q(back_order[step - 3])
    for k in order[1:]:
        r_copies[k].wait_recv()

    returned = back[...].reshape(experts * capacity, lf)
    every = lax.broadcasted_iota(jnp.int32, (count, experts * capacity), 1).astype(F32)
    combined = jnp.zeros((count, lf), F32)
    for k in range(top):
        chosen = jnp.where(every == columns[:, 1 + top + k : 2 + top + k], 1.0, 0.0).astype(BF16)
        combined = combined + columns[:, 1 + k : 2 + k] * jnp.dot(
            chosen, returned, preferred_element_type=F32
        )
    out_ref[...] = (tokens_ref[...].astype(F32) + combined).astype(BF16)
    return router_logsum


def head_part(
    sizes,
    sends,
    weight_copy,
    router_logsum,
    layer_ref,
    gain_ref,
    logsum_ref,
    penalty_ref,
    full,
    weight,
    logits,
    pair,
    pairs,
    square,
    squares,
    layer_sem,
    z_send,
    z_recv,
    g_send,
    g_recv,
    pair_send,
    pair_recv,
    square_send,
    square_recv,
):
    place = Place(sizes)
    X, Z, MP, Y, C = place.X, place.Z, place.MP, place.Y, place.C
    x, z, m, y, c = place.x, place.z, place.m, place.y, place.c
    N = Z * MP
    count, lf = layer_ref.shape
    width = N * lf
    vocabulary = weight.shape[0]

    def block(sz, sm):
        return full.at[:, pl.ds(pl.multiple_of((sz * MP + sm) * lf, lf), lf)]

    order = arrival_order(Z)
    z_copies = {}
    own = pltpu.make_async_copy(layer_ref, block(z, m), layer_sem.at[0])
    own.start()
    for j in order[1:]:
        copy = remote(layer_ref, block(z, m), z_send.at[j], z_recv.at[j], place.z_peer(j))
        copy.start()
        sends.append(copy)
        z_copies[j] = copy

    def sem_at(k, dy, dc):
        return (k * Y + dy) * C + dc

    def source(k, dy, dc):
        sy = lax.rem(y + Y - dy, Y)
        return block(lax.rem(z + Z - k, Z), sy * C + lax.rem(c + C - dc, C))

    def send(k, dy, dc, held, device):
        at = sem_at(k, dy, dc)
        copy = remote(held, held, g_send.at[at], g_recv.at[at], device)
        copy.start()
        sends.append(copy)

    def wait_for(k, dy, dc):
        held = source(k, dy, dc)
        at = sem_at(k, dy, dc)
        remote(held, held, g_send.at[at], g_recv.at[at], place.z_peer(1)).wait_recv()

    def hop_own(k):
        if k == 0:
            own.wait()
        else:
            z_copies[k].wait_recv()
        held = source(k, 0, 0)
        for d in range(1, Y):
            send(k, d, 0, held, place.y_peer(d))
        for d in range(1, C):
            send(k, 0, d, held, place.c_peer(d))

    def hop_y(k):
        for dy in range(1, Y):
            wait_for(k, dy, 0)
            for d in range(1, C):
                send(k, dy, d, source(k, dy, 0), place.c_peer(d))

    def arrive(k):
        for dy in range(Y):
            for dc in range(1, C):
                wait_for(k, dy, dc)

    tile = 256 if vocabulary % 256 == 0 else vocabulary
    chunk = MP * lf

    def multiply(k, begin):
        at = pl.ds(pl.multiple_of(lax.rem(z + Z - k, Z) * chunk, chunk), chunk)
        value = full[:, at].astype(F32)
        held = (value * gain_ref[:, at]).astype(BF16)

        def vocab_tile(t, carry):
            spot = pl.ds(pl.multiple_of(t * tile, tile), tile)
            product = lax.dot_general(weight[spot, at], held, NT, preferred_element_type=F32)
            if not begin:
                product = product + logits[spot, :]
            logits[spot, :] = product
            return carry

        lax.fori_loop(0, vocabulary // tile, vocab_tile, 0)
        return jnp.sum(value * value, axis=1, keepdims=True)

    square_sum = jnp.zeros((count, 1), F32)
    for step in range(Z + 2):
        if step < Z:
            hop_own(order[step])
        if 0 <= step - 1 < Z:
            hop_y(order[step - 1])
        if 0 <= step - 2 < Z:
            if step == 2:
                weight_copy.wait()
            arrive(order[step - 2])
            square_sum = square_sum + multiply(order[step - 2], step == 2)

    scale = lax.rsqrt(
        jnp.transpose(jnp.broadcast_to(square_sum, (count, 128)))[0:1] / width + epsilon
    )
    scaled = logits[...] * scale
    peak = jnp.max(scaled, axis=0, keepdims=True)
    total = jnp.sum(jnp.exp(scaled - peak), axis=0, keepdims=True)
    groups = count // 128
    pair[...] = jnp.zeros_like(pair)
    for g in range(groups):
        pair[g : g + 1] = peak[:, g * 128 : (g + 1) * 128]
        pair[groups + g : groups + g + 1] = total[:, g * 128 : (g + 1) * 128]
    pairs[pl.ds(place.linear, 1)] = pair[...][None]
    pair_copies = []
    for j in range(1, N):
        copy = remote(
            pair, pairs.at[place.linear], pair_send.at[j], pair_recv.at[j], place.plane_peer(j)
        )
        copy.start()
        pair_copies.append(copy)
    for copy in pair_copies:
        copy.wait_recv()
    everything = pairs[...]
    peaks, totals = everything[:, 0:groups, :], everything[:, groups : 2 * groups, :]
    merged = jnp.max(peaks, axis=0)
    logsum = merged + jnp.log(jnp.sum(totals * jnp.exp(peaks - merged[None]), axis=0))
    logsum_ref[...] = logsum
    square[...] = jnp.zeros_like(square)
    square[0:1] = jnp.broadcast_to(
        jnp.sum(router_logsum * router_logsum, axis=1, keepdims=True), (1, square.shape[1])
    )
    square[1:2] = jnp.broadcast_to(
        jnp.sum(jnp.sum(logsum * logsum, axis=1, keepdims=True), axis=0, keepdims=True),
        (1, square.shape[1]),
    )
    squares[pl.ds(x, 1)] = square[...][None]
    square_copies = []
    for j in range(1, X):
        copy = remote(
            square, squares.at[x], square_send.at[j], square_recv.at[j], place.x_peer(j)
        )
        copy.start()
        square_copies.append(copy)
    for copy in square_copies:
        copy.wait_recv()
    total = squares[0]
    for j in range(1, X):
        total = total + squares[j]
    penalty_ref[...] = total / (count * X)
    for copy in sends + pair_copies + square_copies:
        copy.wait_send()


def kernel(sizes, experts, top, capacity, split, *refs):
    layer_in, (head_gain, head_weight) = refs[:8], refs[8:10]
    out_ref, logsum_ref, penalty_ref = refs[10:13]
    layer_scratch, head_scratch = refs[13 : 13 + split], refs[13 + split : -1]
    head_weight_copy = pltpu.make_async_copy(head_weight, head_scratch[1], refs[-1].at[0])
    sends = []
    router_logsum = layer_part(
        sizes, sends, head_weight_copy, experts, top, capacity, *layer_in, out_ref, *layer_scratch
    )
    head_part(
        sizes,
        sends,
        head_weight_copy,
        router_logsum,
        out_ref,
        head_gain,
        logsum_ref,
        penalty_ref,
        *head_scratch,
    )


def body(
    sizes,
    tokens,
    expert_index,
    slot_index,
    norm_gain,
    router_weight,
    gate_weight,
    up_weight,
    down_weight,
    final_gain,
    head_weight,
):
    X, Z, MP = sizes
    C = 2 if MP % 2 == 0 else 1
    Y = MP // C
    N = Z * MP
    count, lf = tokens.shape
    top = expert_index.shape[1]
    experts = router_weight.shape[0]
    capacity = 3 * count // experts
    _, ff, width = gate_weight.shape
    vocabulary = head_weight.shape[0]
    padded = -(-(experts + 1) // 8) * 8
    groups = count // 128
    pair_rows = -(-2 * groups // 8) * 8
    tile = 128 if ff % 128 == 0 else ff
    vmem = pl.BlockSpec(memory_space=pltpu.VMEM)
    anywhere = pl.BlockSpec(memory_space=pl.ANY)
    dma = pltpu.SemaphoreType.DMA
    layer_scratch = [
            pltpu.VMEM((padded, lf), F32),
            pltpu.VMEM((count, 128), F32),
            pltpu.VMEM((ff // tile, 2, X * capacity, tile), F32),
            pltpu.VMEM((padded, count), F32),
            pltpu.VMEM((N, padded, count), F32),
            pltpu.VMEM((128, count), F32),
            pltpu.VMEM((experts, capacity, lf), BF16),
            pltpu.VMEM((X * capacity, width), BF16),
            pltpu.VMEM((ff // tile, 2, tile, width), BF16),
            pltpu.VMEM((ff, width), BF16),
            pltpu.VMEM((X * capacity, ff), BF16),
            pltpu.VMEM((Z, Y, C, X * capacity, lf), BF16),
            pltpu.VMEM((Z, C, Y, X * capacity, lf), BF16),
            pltpu.VMEM((Z, Y, X * capacity, lf), BF16),
            pltpu.VMEM((Z, Y, X, capacity, lf), BF16),
            pltpu.VMEM((Z, X, capacity, lf), BF16),
            pltpu.VMEM((Z, X, capacity, lf), BF16),
            pltpu.VMEM((Z, capacity, lf), BF16),
            pltpu.VMEM((Z, capacity, lf), BF16),
            dma((N,)),
            dma((N,)),
            dma((1,)),
            dma((Z,)),
            dma((Z,)),
            dma((Z * X * Y * C,)),
            dma((Z * X * Y * C,)),
            dma((2 * (ff // tile) + 1,)),
            dma((Z * C,)),
            dma((Z * C,)),
            dma((Z * X * Y,)),
            dma((Z * X * Y,)),
            dma((Z * X,)),
            dma((Z * X,)),
            dma((Z,)),
            dma((Z,)),
    ]
    head_scratch = [
            pltpu.VMEM((count, width), BF16),
            pltpu.VMEM((vocabulary, width), BF16),
            pltpu.VMEM((vocabulary, count), F32),
            pltpu.VMEM((pair_rows, 128), F32),
            pltpu.VMEM((N, pair_rows, 128), F32),
            pltpu.VMEM((8, 128), F32),
            pltpu.VMEM((X, 8, 128), F32),
            dma((1,)),
            dma((Z,)),
            dma((Z,)),
            dma((N,)),
            dma((N,)),
            dma((N,)),
            dma((N,)),
            dma((X,)),
            dma((X,)),
    ]
    layer_out, logsum, penalty = pl.pallas_call(
        functools.partial(kernel, sizes, experts, top, capacity, len(layer_scratch)),
        out_shape=(
            jax.ShapeDtypeStruct((count, lf), BF16),
            jax.ShapeDtypeStruct((groups, 128), F32),
            jax.ShapeDtypeStruct((8, 128), F32),
        ),
        in_specs=[vmem] * 5 + [anywhere] * 3 + [vmem, anywhere],
        out_specs=(vmem, vmem, vmem),
        scratch_shapes=layer_scratch + head_scratch + [dma((1,))],
        compiler_params=pltpu.CompilerParams(
            has_side_effects=True, vmem_limit_bytes=VMEM_LIMIT, collective_id=0
        ),
        name="scoring",
    )(
        tokens,
        expert_index,
        slot_index,
        norm_gain[None, :],
        router_weight,
        gate_weight[0],
        up_weight[0],
        down_weight[0],
        final_gain[None, :],
        head_weight,
    )
    return (layer_out, logsum.reshape(count), penalty[0, 0], penalty[1, 0])


def solution(mesh):
    in_specs = (
        P("dp", ("expert", "mp")),
        P("dp", None),
        P("dp", None),
        P(("expert", "mp")),
        P(None, ("expert", "mp")),
        P("expert", ("dp", "mp"), None),
        P("expert", ("dp", "mp"), None),
        P("expert", ("dp", "mp"), None),
        P(),
        P(("expert", "mp"), None),
    )
    out_specs = (P("dp", ("expert", "mp")), P("dp"), P(), P())
    sizes = (mesh.shape["dp"], mesh.shape["expert"], mesh.shape["mp"])
    return jax.shard_map(
        functools.partial(body, sizes),
        mesh=mesh,
        in_specs=in_specs,
        out_specs=out_specs,
        check_vma=False,
    )
```
